16 devices in a mesh: rep: 1, r: 2 (over z), s: 8 (over x, y, core).
Axes of the slice: x: 2, y: 2, z: 2, core: 2. Of those that a mesh axis runs over, the one named last changes fastest.
Arguments:
- x: bfloat16 [16, 4096, 1024], P(('rep', 'r', 's'))
- dy: bfloat16 [16, 4096, 1024], P(('rep', 'r', 's'))
- w_gate: bfloat16 [2, 1024, 2560], P(None, 's')
- w_up: bfloat16 [2, 1024, 2560], P(None, 's')
- w_down: bfloat16 [2, 2560, 1024], P(None, 's')
- m_w_gate: float32 [2, 1024, 2560], P(None, 's')
- m_w_up: float32 [2, 1024, 2560], P(None, 's')
- m_w_down: float32 [2, 2560, 1024], P(None, 's')
- v_w_gate: float32 [2, 1024, 2560], P(None, 's')
- v_w_up: float32 [2, 1024, 2560], P(None, 's')
- v_w_down: float32 [2, 2560, 1024], P(None, 's')
Outputs:
- output 1: bfloat16 [2, 1024, 2560], P('rep', 's')
- output 2: bfloat16 [2, 1024, 2560], P('rep', 's')
- output 3: bfloat16 [2, 2560, 1024], P('rep', 's')
- output 4: float32 [2, 1024, 2560], P('rep', 's')
- output 5: float32 [2, 1024, 2560], P('rep', 's')
- output 6: float32 [2, 2560, 1024], P('rep', 's')
- output 7: float32 [2, 1024, 2560], P('rep', 's')
- output 8: float32 [2, 1024, 2560], P('rep', 's')
- output 9: float32 [2, 2560, 1024], P('rep', 's')
All inputs are finite; a program needn't handle non-finite values.
Results may differ from the reference program's by a relative error of at most 0.022.
Values are sent between devices in bfloat16 or wider.
A program may use at most 2 GiB of HBM per device.

```python
import jax
import jax.numpy as jnp
from jax import lax

SEQUENCES = 16
TOKENS = 4096
D = 1024
FF = 2560
LAYERS = 2
NAMES = ("w_gate", "w_up", "w_down")
SHAPES = {"w_gate": (LAYERS, D, FF), "w_up": (LAYERS, D, FF), "w_down": (LAYERS, FF, D)}


def bump(key, n, height):
    away = (jnp.arange(n, dtype=jnp.int32) - jax.random.randint(key, (), 0, n, jnp.int32)) % n
    return jnp.where(away < n // 8, height, 1.0)


def together(key, own, strength):
    shared = jax.random.normal(key, own.shape[1:], jnp.float32)
    return (own + strength * shared) * lax.rsqrt(1 + strength * strength)


def setup_inputs(seed: int = 0, part: int = 0) -> dict:
    kx, kdy, ka, kb, kz, kf, kh, kl, *keys = jax.random.split(jax.random.key(seed), 8 + 3 * len(NAMES))
    kx, kdy, ka, kb = (jax.random.fold_in(k, part) for k in (kx, kdy, ka, kb))
    kw, km, kv = (keys[i::3] for i in range(3))
    shape = (SEQUENCES, TOKENS, D)
    much_x, much_dy = jax.random.uniform(kz, (2,), jnp.float32, 0.0, 1.0)
    loud = 2.0 ** jax.random.uniform(jax.random.fold_in(kz, 1), (), jnp.float32, -1.0, 2.0)
    layers = 2.0 ** jax.random.uniform(kl, (LAYERS, 1, 1), jnp.float32, -1.0, 1.0)
    x = together(ka, jax.random.normal(kx, shape, jnp.float32), much_x) * bump(kf, D, 4.0)
    dy = together(kb, jax.random.normal(kdy, shape, jnp.float32), much_dy)
    drawn = {"x": x.astype(jnp.bfloat16), "dy": (loud * dy * (SEQUENCES * TOKENS) ** -0.5).astype(jnp.bfloat16)}
    for key, name in zip(kw, NAMES, strict=True):
        w = jax.random.normal(key, SHAPES[name], jnp.float32) * SHAPES[name][1] ** -0.5
        drawn[name] = (w * {"w_gate": 1.0, "w_up": bump(kh, FF, 4.0), "w_down": layers}[name]).astype(jnp.bfloat16)
    for key, name in zip(km, NAMES, strict=True):
        drawn[f"m_{name}"] = 0.1 * jax.random.normal(key, SHAPES[name], jnp.float32)
    for key, name in zip(kv, NAMES, strict=True):
        drawn[f"v_{name}"] = jax.random.uniform(key, SHAPES[name], jnp.float32, 0.005, 0.015)
    return drawn


def matmul(a, w):
    return jnp.dot(a, w, preferred_element_type=jnp.float32).astype(jnp.bfloat16)


def normed(h):
    wide = h.astype(jnp.float32)
    scale = lax.rsqrt(jnp.mean(wide**2, -1, keepdims=True) + 1e-6)
    return (wide * scale).astype(jnp.bfloat16)


def layer(h, w):
    a = normed(h)
    gate = jnp.dot(a, w["w_gate"], preferred_element_type=jnp.float32)
    up = jnp.dot(a, w["w_up"], preferred_element_type=jnp.float32)
    return h + matmul((jax.nn.silu(gate) * up).astype(jnp.bfloat16), w["w_down"])


def adamw(w, m, v, g):
    m = 0.9 * m + 0.1 * g
    v = 0.95 * v + 0.05 * g * g
    step = m * lax.rsqrt(v + 1e-8) + 0.1 * w
    return (w - 0.02 * step).astype(jnp.bfloat16), m, v


def clipped(gradients, sum_of_squares, count):
    factor = jnp.minimum(1.0, 0.5 * lax.rsqrt(sum_of_squares / count + 1e-30))
    return [g * factor for g in gradients]


def stack(weights, h):
    return lax.scan(lambda h, w: (layer(h, w), None), h, weights)[0]


def reference(x, dy, w_gate, w_up, w_down, m_w_gate, m_w_up, m_w_down, v_w_gate, v_w_up, v_w_down):
    weights = dict(zip(NAMES, (w_gate, w_up, w_down), strict=True))

    def take(so_far, sequence):
        h, by_y = sequence
        _, back = jax.vjp(lambda w: stack(w, h), weights)
        return jax.tree.map(lambda total, term: total + term.astype(jnp.float32), so_far, back(by_y)[0]), None

    none_yet = {name: jnp.zeros(w.shape, jnp.float32) for name, w in weights.items()}
    by_weights, _ = lax.scan(take, none_yet, (x, dy))
    gradients = [by_weights[name].astype(jnp.bfloat16).astype(jnp.float32) for name in NAMES]
    gradients = clipped(gradients, sum(jnp.sum(g * g) for g in gradients), sum(g.size for g in gradients))
    new = [
        adamw(w.astype(jnp.float32), m, v, g)
        for w, m, v, g in zip((w_gate, w_up, w_down), (m_w_gate, m_w_up, m_w_down), (v_w_gate, v_w_up, v_w_down), gradients, strict=True)
    ]
    return tuple(one[which] for which in range(3) for one in new)
```

```python
import functools

import jax
import jax.numpy as jnp
from jax import lax
from jax.experimental import pallas as pl
from jax.experimental.pallas import tpu as pltpu
from jax.sharding import PartitionSpec as P

BF, F32 = jnp.bfloat16, jnp.float32
T, D, FF = 4096, 1024, 2560
NJ, FB = 5, 512
TT = 1024
LAST = T // TT - 1
VMEM_LIMIT = 63 * 1024 * 1024
NN = (((1,), (0,)), ((), ()))
NT = (((1,), (1,)), ((), ()))


def dot(a, b, dims=NN):
    return lax.dot_general(a, b, dims, preferred_element_type=F32)


def call(kernel, flops, nbytes, **kw):
    return pl.pallas_call(
        kernel,
        cost_estimate=pl.CostEstimate(flops=int(flops), bytes_accessed=int(nbytes), transcendentals=0),
        compiler_params=pltpu.CompilerParams(vmem_limit_bytes=VMEM_LIMIT),
        **kw,
    )


def norm_scale(wide):
    return lax.rsqrt(jnp.mean(wide * wide, -1, keepdims=True) + 1e-6)


def flip(me, k):
    out = me
    for bit in (1, 2, 4):
        if k & bit:
            out = out + bit - 2 * bit * lax.rem(lax.div(out, bit), 2)
    return out


def forward_kernel(
    x_ref, dy_ref, wg_hbm, wu_hbm, wd_hbm, at_ref, dyt_ref, g_ref, u_ref, hid_ref, wd_full, a_all, wg, wu, sems, rsems, own_sems
):
    me = lax.axis_index("s")
    j, t = pl.program_id(0), pl.program_id(1)

    def copies(c, m):
        first, second = ((4, 2), (2, 4))[m]

        def part(ref, k, whole):
            if c is None:
                return ref.at[pl.ds(0 if whole else pl.multiple_of(flip(me, k) * 320, 64), 320), pl.ds(512 * m, 512)]
            return ref.at[pl.ds(0 if whole else pl.multiple_of(flip(me, k) * 128, 128), 128), pl.ds(pl.multiple_of(c * FB, FB), FB)]

        full = wd_full if c is None else (wg, wu)[m]
        mine = wd_hbm.at[0] if c is None else (wg_hbm, wu_hbm)[m].at[0]
        n = NJ if c is None else c

        def copy(i, k, to):
            src = part(mine, 0, True) if k == 0 else part(full, k, False)
            return lambda: pltpu.make_async_remote_copy(
                src_ref=src, dst_ref=part(full, k, False), send_sem=sems.at[n, m, i], recv_sem=rsems.at[n, m, i],
                device_id={"s": flip(me, to)}, device_id_type=pl.DeviceIdType.MESH,
            )

        direct = [copy(0, 0, first), copy(1, 0, second), copy(2, 0, 1)]
        forward = [copy(3, first, second)]
        core = [copy(4, first, 1), copy(5, second, 1)], [copy(6, 6, 1)]
        return direct, forward, core

    def each(c, do):
        for m in range(2):
            do(*copies(c, m))

    def starts(cs):
        for x in cs:
            x().start()

    def begin(c):
        each(c, lambda direct, forward, core: starts(direct))

    def onward(c):
        def do(direct, forward, core):
            for x in direct[:2]:
                x().wait_recv()
            starts(forward)
            starts(core[0])

        each(c, do)

    def across(c):
        def do(direct, forward, core):
            forward[0]().wait_recv()
            starts(core[1])

        each(c, do)

    def here(c):
        def do(direct, forward, core):
            for x in direct[2:] + core[0] + core[1]:
                x().wait_recv()

        each(c, do)

    def sent(c):
        def do(direct, forward, core):
            for x in direct + forward + core[0] + core[1]:
                x().wait_send()

        each(c, do)

    def own():
        rows = pl.ds(pl.multiple_of(me * 128, 128), 128)
        down_rows = pl.ds(pl.multiple_of(me * 320, 64), 320)
        return [
            lambda: pltpu.make_async_copy(wg_hbm.at[0], wg.at[rows], own_sems.at[0]),
            lambda: pltpu.make_async_copy(wu_hbm.at[0], wu.at[rows], own_sems.at[1]),
            lambda: pltpu.make_async_copy(wd_hbm.at[0], wd_full.at[down_rows], own_sems.at[2]),
        ]

    @pl.when((j == 0) & (t == 0))
    def _():
        barrier = pltpu.get_barrier_semaphore()
        for k in (1, 2, 4):
            pl.semaphore_signal(barrier, inc=1, device_id={"s": flip(me, k)}, device_id_type=pl.DeviceIdType.MESH)
        pl.semaphore_wait(barrier, 3)
        begin(0)
        starts(own())

    @pl.when(j == 0)
    def _():
        wide = x_ref[...].astype(F32)
        a = (wide * norm_scale(wide)).astype(BF)
        a_all[pl.ds(pl.multiple_of(t * TT, TT), TT), :] = a
        at_ref[...] = a.T
        dyt_ref[...] = dy_ref[...].T

    @pl.when(((j == 0) & (t == 2)) | ((j > 0) & (j < NJ) & (t == 0)))
    def _():
        onward(j)

        @pl.when(j < NJ - 1)
        def _():
            begin(j + 1)

        @pl.when(j == NJ - 1)
        def _():
            begin(None)

    @pl.when(((j == 0) & (t == LAST)) | ((j > 0) & (j < NJ) & (t == 2)))
    def _():
        across(j)

    @pl.when((j < NJ) & (t == LAST))
    def _():
        here(j)

    @pl.when((j == 0) & (t == LAST))
    def _():
        for x in own():
            x().wait()

    @pl.when((j == NJ) & (t == 1))
    def _():
        onward(None)

    @pl.when(j > 0)
    def _():
        a = a_all[pl.ds(pl.multiple_of(t * TT, TT), TT), :]
        cols = pl.ds(pl.multiple_of((j - 1) * FB, FB), FB)
        g = dot(a, wg[:, cols])
        u = dot(a, wu[:, cols])
        g_ref[...] = g
        u_ref[...] = u
        hid_ref[...] = (g * jax.nn.sigmoid(g) * u).astype(BF)

    @pl.when((j == NJ) & (t == LAST))
    def _():
        across(None)
        here(None)
        sent(None)
        lax.fori_loop(0, NJ, lambda c, _: (sent(c), 0)[1], 0)


def forward(x, dy, wg, wu, wd):
    rows = pl.BlockSpec((TT, D), lambda j, t: (jnp.where(j == 0, t, LAST), 0))
    cols = pl.BlockSpec((D, TT), lambda j, t: (0, jnp.where(j == 0, t, LAST)))
    tile = pl.BlockSpec((TT, FB), lambda j, t: (jnp.where(j == 0, 0, t), jnp.maximum(j - 1, 0)))
    anywhere = pl.BlockSpec(memory_space=pl.ANY)
    sems = pltpu.SemaphoreType.DMA((NJ + 1, 2, 7))
    return pl.pallas_call(
        forward_kernel,
        cost_estimate=pl.CostEstimate(flops=4 * T * D * FF, bytes_accessed=10 * T * FF, transcendentals=0),
        compiler_params=pltpu.CompilerParams(vmem_limit_bytes=VMEM_LIMIT, collective_id=3, has_side_effects=True),
        name="forward", grid=(NJ + 1, T // TT),
        in_specs=[rows, rows] + [anywhere] * 3, out_specs=[cols, cols, tile, tile, tile, anywhere],
        out_shape=[
            jax.ShapeDtypeStruct((D, T), BF), jax.ShapeDtypeStruct((D, T), BF), jax.ShapeDtypeStruct((T, FF), F32),
            jax.ShapeDtypeStruct((T, FF), F32), jax.ShapeDtypeStruct((T, FF), BF), jax.ShapeDtypeStruct((FF, D), BF),
        ],
        scratch_shapes=[
            pltpu.VMEM((T, D), BF), pltpu.VMEM((D, FF), BF), pltpu.VMEM((D, FF), BF), sems, sems, pltpu.SemaphoreType.DMA((3,)),
        ],
    )(x, dy, wg, wu, wd)


def down_kernel(hid_ref, x_ref, wd_ref, h_ref, a_ref, at_ref):
    h = x_ref[...] + dot(hid_ref[...], wd_ref[...]).astype(BF)
    h_ref[...] = h
    wide = h.astype(F32)
    a = (wide * norm_scale(wide)).astype(BF)
    a_ref[...] = a
    at_ref[...] = a.T


def down(hid, x, wd):
    rows = pl.BlockSpec((512, D), lambda t: (t, 0))
    return call(
        down_kernel, 2 * T * D * FF, 2 * T * FF + 8 * T * D, name="down", grid=(T // 512,),
        in_specs=[pl.BlockSpec((512, FF), lambda t: (t, 0)), rows, pl.BlockSpec((FF, D), lambda t: (0, 0))],
        out_specs=[rows, rows, pl.BlockSpec((D, 512), lambda t: (0, t))],
        out_shape=[jax.ShapeDtypeStruct((T, D), BF), jax.ShapeDtypeStruct((T, D), BF), jax.ShapeDtypeStruct((D, T), BF)],
    )(hid, x, wd)


def cat(refs):
    return jnp.concatenate([r[...] for r in refs], axis=1)


def comm_scratch(chunks):
    blocks = (2, 2, 384, 512)
    return [
        pltpu.VMEM(blocks, F32),
        pltpu.VMEM(blocks, BF),
        pltpu.VMEM((2, *blocks), BF),
        pltpu.VMEM((2, 2, 192, 512), BF),
        pltpu.VMEM((2, 2, 2, 192, 512), BF),
        pltpu.VMEM((2, 192, 512), BF),
        pltpu.VMEM((2, 2, 192, 512), BF),
        pltpu.VMEM((384, 512), BF),
        pltpu.VMEM((2, 384, 512), BF),
        pltpu.SemaphoreType.DMA((6,)),
        pltpu.SemaphoreType.DMA((6, 2)),
    ]


def exchange(me, peer, keep, send1, recv1, send2, recv2, send3, recv3, send4, recv4, sems, rsems, out_ref):
    one, two, four = ({"s": flip(me, k)} for k in (1, 2, 4))
    z = {"r": peer}

    def copy(i, src, dst, slot, to):
        return pltpu.make_async_remote_copy(
            src_ref=src, dst_ref=dst, send_sem=sems.at[i], recv_sem=rsems.at[i, slot], device_id=to, device_id_type=pl.DeviceIdType.MESH
        )

    def c1(slot):
        return [copy(0, send1, recv1.at[slot], slot, one)]

    def c2(slot):
        return [copy(1 + i, send2.at[i], recv2.at[slot, i], slot, to) for i, to in enumerate((four, two))]

    def c3(slot):
        return [copy(3 + i, send3.at[i], recv3.at[slot, i], slot, to) for i, to in enumerate((two, four))]

    def c4(slot):
        return [copy(5, send4, recv4.at[slot], slot, z)]

    def start(cs):
        for c in cs:
            c.start()

    def wait(cs):
        for c in cs:
            c.wait()

    lo, hi = slice(0, 192), slice(192, 384)

    def s1(slot):
        start(c1(slot))

    def s2(slot):
        wait(c1(slot))
        for k in range(2):
            def total(kx, ky, rows):
                return keep[kx, ky, rows] + recv1[slot, kx, ky, rows].astype(F32)

            send2[0, k] = total(1, k, lo).astype(BF)
            send2[1, k] = total(k, 1, hi).astype(BF)
            keep[0, k, lo] = total(0, k, lo)
            keep[k, 0, hi] = total(k, 0, hi)
        start(c2(slot))

    def s3(slot):
        wait(c2(slot))
        send3[0] = (keep[0, 1, lo] + recv2[slot, 0, 1].astype(F32)).astype(BF)
        send3[1] = (keep[1, 0, hi] + recv2[slot, 1, 1].astype(F32)).astype(BF)
        keep[0, 0, lo] = keep[0, 0, lo] + recv2[slot, 0, 0].astype(F32)
        keep[0, 0, hi] = keep[0, 0, hi] + recv2[slot, 1, 0].astype(F32)
        start(c3(slot))

    def s4(slot):
        wait(c3(slot))
        send4[lo] = (keep[0, 0, lo] + recv3[slot, 0].astype(F32)).astype(BF)
        send4[hi] = (keep[0, 0, hi] + recv3[slot, 1].astype(F32)).astype(BF)
        start(c4(slot))

    def final(e, slot):
        wait(c4(slot))
        out_ref[e] = (send4[...].astype(F32) + recv4[slot].astype(F32)).astype(BF)

    return s1, s2, s3, s4, final


def grads_kernel(second, *refs):
    if second:
        a_ref, *refs = refs
        wg, wu, refs = refs[:4], refs[4:8], refs[8:]
        dy_ref, at_ref, dyt_ref, wd_ref, out_ref, dg_ref, du_ref, hkeep, hsend, accg, accu, accd, down_ref, hsems, *comm = refs
    else:
        g_refs, u_refs, refs = refs[:4], refs[4:8], refs[8:]
        dy_ref, at_ref, dyt_ref, wd_ref, hkeep, hsend, out_ref, accg, accu, accd, down_ref, hsems, *comm = refs
    keep, send1 = comm[:2]
    me, group = lax.axis_index("s"), lax.axis_index("r")
    j, t = pl.program_id(0), pl.program_id(1)
    last = pl.num_programs(1) - 1
    off = 0 if second else 1
    s1, s2, s3, s4, final = exchange(me, 1 - group, *comm, out_ref)

    @pl.when((j == 0) & (t == 0))
    def _():
        barrier = pltpu.get_barrier_semaphore()
        for to in [{"s": flip(me, k)} for k in (1, 2, 4)] + [{"r": 1 - group}]:
            pl.semaphore_signal(barrier, inc=1, device_id=to, device_id_type=pl.DeviceIdType.MESH)
        pl.semaphore_wait(barrier, 4)
        if not second:
            hands = [pltpu.make_async_copy(hkeep, keep, hsems.at[0]), pltpu.make_async_copy(hsend, send1, hsems.at[1])]
            for h in hands:
                h.start()
            for h in hands:
                h.wait()
            s1(0)

    @pl.when(t == 0)
    def _():
        for acc in (accg, accu, accd):
            acc[...] = jnp.zeros_like(acc)

    def front(i):
        two = slice(2 * i, 2 * i + 2)
        cols = slice(256 * i, 256 * (i + 1))
        if second:
            a = a_ref[...]
            g, u = dot(a, cat(wg[two])), dot(a, cat(wu[two]))
        else:
            g, u = cat(g_refs[two]), cat(u_refs[two])
        dh = dot(dy_ref[...], wd_ref[two].reshape(256, D), NT).astype(BF).astype(F32)
        s = jax.nn.sigmoid(g)
        silu = g * s
        hid = (silu * u).astype(BF)
        du = (dh * silu).astype(BF)
        dg = (dh * u * (s + silu * (1.0 - s))).astype(BF)
        if second:
            dg_ref[:, cols] = dg
            du_ref[:, cols] = du
        return hid, dg, du

    def back(i, hid, dg, du):
        cols = slice(256 * i, 256 * (i + 1))
        accg[:, cols] += dot(at_ref[...], dg)
        accu[:, cols] += dot(at_ref[...], du)
        accd[:, cols] += dot(dyt_ref[...], hid)

    zero, one = front(0), front(1)
    back(0, *zero)
    back(1, *one)

    e = j - 1 + off
    slot = lax.rem(e + 2, 2)
    for at_t, stage in ((0, s2), (2, s3), (3, s4)):
        @pl.when((t == at_t) & (e >= 0))
        def _():
            stage(slot)

    @pl.when((t == 1) & (e >= 1))
    def _():
        final(e - 1, lax.rem(e + 1, 2))

    @pl.when(t == last)
    def _():
        down_ref[...] = accd[...].T
        for k in range(8):
            out = (keep, send1)[k % 2]
            kx, ky = k // 4, k // 2 % 2
            d = flip(me, k)
            wide = pl.ds(pl.multiple_of(d * 128, 128), 128)
            rows = pl.ds(pl.multiple_of(d * 64, 64), 64)
            out[kx, ky, 0:128] = accg[wide, :].astype(out.dtype)
            out[kx, ky, 128:256] = accu[wide, :].astype(out.dtype)
            out[kx, ky, 256:320] = down_ref[rows, 0:512].astype(out.dtype)
            out[kx, ky, 320:384] = down_ref[rows, 512:1024].astype(out.dtype)

    new = lax.rem(e + 3, 2)
    end = (t == last) & (j == NJ - 1)
    if second:
        @pl.when((t == last) & (j < NJ - 1))
        def _():
            s1(new)

        @pl.when(end)
        def _():
            hands = [pltpu.make_async_copy(keep, hkeep, hsems.at[0]), pltpu.make_async_copy(send1, hsend, hsems.at[1])]
            for h in hands:
                h.start()
            final(NJ - 2, (NJ - 2) % 2)
            for h in hands:
                h.wait()
    else:
        @pl.when(t == last)
        def _():
            s1(new)

        @pl.when(end)
        def _():
            final(NJ - 1, (NJ - 1) % 2)
            for stage in (s2, s3, s4):
                stage(NJ % 2)
            final(NJ, NJ % 2)


def grads(gate_up_of, dy, at, dyt, wd, handed=None):
    second = handed is None
    rows = pl.BlockSpec((TT, D), lambda j, t: (t, 0))
    cols = pl.BlockSpec((D, TT), lambda j, t: (0, t))
    if second:
        a, wg, wu = gate_up_of
        wspec = [pl.BlockSpec((D, 128), lambda j, t, c=c: (0, 5 * c + j)) for c in range(4)]
        ops, specs = [a] + [wg] * 4 + [wu] * 4, [rows] + wspec * 2
    else:
        g, u = gate_up_of
        gspec = [pl.BlockSpec((TT, 128), lambda j, t, c=c: (t, 5 * c + j)) for c in range(4)]
        ops, specs = [g] * 4 + [u] * 4, gspec * 2
    chunks = NJ - 1 if second else NJ + 1
    ops += [dy, at, dyt, wd.reshape(4, NJ, 128, D)]
    specs += [rows, cols, cols, pl.BlockSpec((4, 1, 128, D), lambda j, t: (0, j, 0, 0))]
    outs = [jax.ShapeDtypeStruct((chunks, 384, 512), BF)]
    ospecs = [pl.BlockSpec((chunks, 384, 512), lambda j, t: (0, 0, 0))]
    hand = [jax.ShapeDtypeStruct((2, 2, 384, 512), F32), jax.ShapeDtypeStruct((2, 2, 384, 512), BF)]
    anywhere = [pl.BlockSpec(memory_space=pl.ANY)] * 2
    if second:
        outs += [jax.ShapeDtypeStruct((T, FF), BF)] * 2 + hand
        ospecs += [pl.BlockSpec((TT, FB), lambda j, t: (t, j))] * 2 + anywhere
    else:
        ops += handed
        specs += anywhere
    return pl.pallas_call(
        functools.partial(grads_kernel, second),
        cost_estimate=pl.CostEstimate(flops=(12 if second else 8) * T * D * FF, bytes_accessed=40 * T * D * NJ, transcendentals=0),
        compiler_params=pltpu.CompilerParams(vmem_limit_bytes=VMEM_LIMIT, collective_id=1 if second else 2, has_side_effects=True),
        name="grads_second" if second else "grads_first", grid=(NJ, T // TT),
        in_specs=specs, out_specs=ospecs, out_shape=outs,
        scratch_shapes=[pltpu.VMEM((D, FB), F32)] * 3 + [pltpu.VMEM((FB, D), F32), pltpu.SemaphoreType.DMA((2,))] + comm_scratch(chunks),
    )(*ops)


def dstate_kernel(groups, *refs):
    n = len(groups)
    dgs, dus, (h_ref, dy_ref, wg_ref, wu_ref, dh_ref, dht_ref) = refs[:n], refs[n : 2 * n], refs[2 * n :]

    def back(parts, w_ref):
        total, j = None, 0
        for ref, count in zip(parts, groups, strict=True):
            for k in range(count):
                w = jnp.concatenate([w_ref[:, 128 * (5 * c + j) : 128 * (5 * c + j + 1)] for c in range(4)], axis=1)
                one = dot(ref[:, FB * k : FB * (k + 1)], w, NT)
                total = one if total is None else total + one
                j += 1
        return total.astype(BF)

    da = (back(dgs, wg_ref) + back(dus, wu_ref)).astype(F32)
    wide = h_ref[...].astype(F32)
    scale = norm_scale(wide)
    along = jnp.sum(da * wide, -1, keepdims=True)
    dn = (da * scale - wide * (along * scale * scale * scale * (1.0 / D))).astype(BF)
    dh = dy_ref[...] + dn
    dh_ref[...] = dh
    dht_ref[...] = dh.T


def dstate(dgs, dus, h, dy, wg, wu):
    groups = tuple(d.shape[1] // FB for d in dgs)
    tt = 512
    rows = pl.BlockSpec((tt, D), lambda t: (t, 0))
    wide = [pl.BlockSpec((tt, FB * n), lambda t: (t, 0)) for n in groups]
    w = pl.BlockSpec((D, FF), lambda t: (0, 0))
    return call(
        functools.partial(dstate_kernel, groups), 4 * T * D * FF, 4 * T * FF + 8 * T * D, name="dstate", grid=(T // tt,),
        in_specs=wide * 2 + [rows, rows, w, w],
        out_specs=[rows, pl.BlockSpec((D, tt), lambda t: (0, t))],
        out_shape=[jax.ShapeDtypeStruct((T, D), BF), jax.ShapeDtypeStruct((D, T), BF)],
    )(*dgs, *dus, h, dy, wg, wu)


def adamw(w, m, v, g):
    m = 0.9 * m + 0.1 * g
    v = 0.95 * v + 0.05 * g * g
    step = m * lax.rsqrt(v + 1e-8) + 0.1 * w
    return (w - 0.02 * step).astype(BF), m, v


def solution(mesh):
    size = mesh.shape["s"]

    def swap(v, k):
        return lax.ppermute(v, "s", [(i, i ^ k) for i in range(size)])

    def gradients_of(parts):
        whole = jnp.concatenate(parts, axis=0)
        gate, up = (
            whole[:, 128 * i : 128 * (i + 1)].reshape(NJ, 128, 4, 128).transpose(1, 2, 0, 3).reshape(128, FF) for i in range(2)
        )
        rows = jnp.concatenate([whole[:, 256:320], whole[:, 320:384]], axis=2)
        core = lax.axis_index("s") % 2
        mine = jnp.where(core == 0, rows[:3], rows[2:])
        other = swap(jnp.where(core == 0, rows[3:], rows[:2]), 1)
        units = jnp.stack([mine[0], other[0], mine[1], other[1], mine[2]])
        return gate, up, units.reshape(320, D)

    def fetched(weights, number):
        return [lax.all_gather(w[number], "s", axis=0, tiled=True) for w in weights]

    def step(x, dy, *arrays):
        weights, m, v = (arrays[i : i + 3] for i in (0, 3, 6))
        x, dy = x[0], dy[0]
        wg1, wu1, wd1 = fetched(weights, 1)
        a0t, dyt, g0, u0, hid0, wd0 = forward(x, dy, *weights)
        h1, a1, a1t = down(hid0, x, wd0)
        done1, dg, du, *handed = grads((a1, wg1, wu1), dy, a1t, dyt, wd1)
        dh1, dh1t = dstate([dg], [du], h1, dy, wg1, wu1)
        done0, = grads((g0, u0), dh1, a0t, dh1t, wd0, handed)
        parts1, parts0 = [done1, done0[:1]], [done0[1:]]
        both = [gradients_of(parts0), gradients_of(parts1)]
        gs = [[both[l][i].astype(F32) for l in range(2)] for i in range(3)]
        squares = lax.psum(sum(jnp.sum(g * g) for pair in gs for g in pair), "s")
        factor = jnp.minimum(1.0, 0.5 * lax.rsqrt(squares / (3 * 2 * D * FF) + 1e-30))
        new = [
            adamw(w.astype(F32), mm, vv, jnp.stack(g) * factor) for w, mm, vv, g in zip(weights, m, v, gs, strict=True)
        ]
        return tuple(one[which] for which in range(3) for one in new)

    states, cut = P(("rep", "r", "s"), None, None), P(None, "s", None)
    return jax.shard_map(
        step, mesh=mesh, in_specs=(states, states) + (cut,) * 9, out_specs=(P("rep", "s", None),) * 9, check_vma=False,
    )
```

```python
import functools

import jax
import jax.numpy as jnp
from jax import lax
from jax.experimental import pallas as pl
from jax.experimental.pallas import tpu as pltpu
from jax.sharding import PartitionSpec as P

BF, F32 = jnp.bfloat16, jnp.float32
T, D, FF = 4096, 1024, 2560
NJ, FB = 5, 512
TT = 1024
LAST = T // TT - 1
VMEM_LIMIT = 63 * 1024 * 1024
NN = (((1,), (0,)), ((), ()))
NT = (((1,), (1,)), ((), ()))


def dot(a, b, dims=NN):
    return lax.dot_general(a, b, dims, preferred_element_type=F32)


def call(kernel, flops, nbytes, **kw):
    return pl.pallas_call(
        kernel,
        cost_estimate=pl.CostEstimate(flops=int(flops), bytes_accessed=int(nbytes), transcendentals=0),
        compiler_params=pltpu.CompilerParams(vmem_limit_bytes=VMEM_LIMIT),
        **kw,
    )


def norm_scale(wide):
    return lax.rsqrt(jnp.mean(wide * wide, -1, keepdims=True) + 1e-6)


def flip(me, k):
    out = me
    for bit in (1, 2, 4):
        if k & bit:
            out = out + bit - 2 * bit * lax.rem(lax.div(out, bit), 2)
    return out


def block(ref, rows, first, cols):
    return ref.at[pl.ds(rows, first), cols]


class Gather:
    def __init__(self, me, mine, full, order, sems, rsems):
        first, second = order

        def copy(i, k, to):
            return lambda: pltpu.make_async_remote_copy(
                src_ref=mine if k == 0 else full(k), dst_ref=full(k), send_sem=sems.at[i], recv_sem=rsems.at[i],
                device_id={"s": flip(me, to)}, device_id_type=pl.DeviceIdType.MESH,
            )

        self.direct = [copy(0, 0, first), copy(1, 0, second), copy(2, 0, 1)]
        self.forward = [copy(3, first, second)]
        self.core1 = [copy(4, first, 1), copy(5, second, 1)]
        self.core2 = [copy(6, 6, 1)]


def starts(cs):
    for c in cs:
        c().start()


def begin(gathers):
    for g in gathers:
        starts(g.direct)


def onward(gathers):
    for g in gathers:
        for c in g.direct[:2]:
            c().wait_recv()
        starts(g.forward)
        starts(g.core1)


def across(gathers):
    for g in gathers:
        g.forward[0]().wait_recv()
        starts(g.core2)


def here(gathers):
    for g in gathers:
        for c in g.direct[2:] + g.core1 + g.core2:
            c().wait_recv()


def sent(gathers):
    for g in gathers:
        for c in g.direct + g.forward + g.core1 + g.core2:
            c().wait_send()


def greet(me, others):
    barrier = pltpu.get_barrier_semaphore()
    for to in others:
        pl.semaphore_signal(barrier, inc=1, device_id=to, device_id_type=pl.DeviceIdType.MESH)
    pl.semaphore_wait(barrier, len(others))


ORDER = ((4, 2), (2, 4))


def forward_kernel(
    x_ref, dy_ref, wg_hbm, wu_hbm, wd_hbm, at_ref, dyt_ref, g_ref, u_ref, hid_ref, wd_full, wd_next, a_all, wg, wu, sems, rsems, own_sems
):
    me = lax.axis_index("s")
    j, t = pl.program_id(0), pl.program_id(1)

    def chunk(c):
        cols = pl.ds(pl.multiple_of(c * FB, FB), FB)
        out = []
        for m in range(4):
            if m < 2:
                mine = (wg_hbm, wu_hbm)[m].at[0, :, cols]
                full = lambda k, m=m: block((wg, wu)[m], pl.multiple_of(flip(me, k) * 128, 128), 128, cols)
            else:
                half = pl.ds(512 * (m - 2), 512)
                mine = wd_hbm.at[0, pl.ds(pl.multiple_of(c * 64, 64), 64), half]
                full = lambda k, half=half: block(wd_full, pl.multiple_of(flip(me, k) * 320 + c * 64, 64), 64, half)
            out.append(Gather(me, mine, full, ORDER[m % 2], sems.at[c, m], rsems.at[c, m]))
        return out

    following = []
    for m in range(2):
        half = pl.ds(512 * m, 512)
        full = lambda k, half=half: block(wd_next, pl.multiple_of(flip(me, k) * 320, 64), 320, half)
        following.append(Gather(me, wd_hbm.at[1, :, half], full, ORDER[m], sems.at[NJ, m], rsems.at[NJ, m]))

    rows = pl.ds(pl.multiple_of(me * 128, 128), 128)
    down_rows = pl.ds(pl.multiple_of(me * 320, 64), 320)
    own = [
        lambda: pltpu.make_async_copy(wg_hbm.at[0], wg.at[rows], own_sems.at[0]),
        lambda: pltpu.make_async_copy(wu_hbm.at[0], wu.at[rows], own_sems.at[1]),
        lambda: pltpu.make_async_copy(wd_hbm.at[0], wd_full.at[down_rows], own_sems.at[2]),
        lambda: pltpu.make_async_copy(wd_hbm.at[1], wd_next.at[down_rows], own_sems.at[3]),
    ]

    @pl.when((j == 0) & (t == 0))
    def _():
        greet(me, [{"s": flip(me, k)} for k in (1, 2, 4)])
        begin(chunk(0))
        starts(own)

    @pl.when(j == 0)
    def _():
        wide = x_ref[...].astype(F32)
        a = (wide * norm_scale(wide)).astype(BF)
        a_all[pl.ds(pl.multiple_of(t * TT, TT), TT), :] = a
        at_ref[...] = a.T
        dyt_ref[...] = dy_ref[...].T

    @pl.when(((j == 0) & (t == 2)) | ((j > 0) & (j < NJ) & (t == 0)))
    def _():
        onward(chunk(j))

        @pl.when(j < NJ - 1)
        def _():
            begin(chunk(j + 1))

        @pl.when(j == NJ - 1)
        def _():
            begin(following)

    @pl.when(((j == 0) & (t == LAST)) | ((j > 0) & (j < NJ) & (t == 2)))
    def _():
        across(chunk(j))

    @pl.when((j < NJ) & (t == LAST))
    def _():
        here(chunk(j))

    @pl.when((j == 0) & (t == LAST))
    def _():
        for c in own:
            c().wait()

    @pl.when((j == NJ) & (t == 1))
    def _():
        onward(following)

    @pl.when(j > 0)
    def _():
        a = a_all[pl.ds(pl.multiple_of(t * TT, TT), TT), :]
        cols = pl.ds(pl.multiple_of((j - 1) * FB, FB), FB)
        g = dot(a, wg[:, cols])
        u = dot(a, wu[:, cols])
        g_ref[...] = g
        u_ref[...] = u
        hid_ref[...] = (g * jax.nn.sigmoid(g) * u).astype(BF)

    @pl.when((j == NJ) & (t == LAST))
    def _():
        across(following)
        here(following)
        sent(following)
        lax.fori_loop(0, NJ, lambda c, _: (sent(chunk(c)), 0)[1], 0)


def forward(x, dy, wg, wu, wd):
    rows = pl.BlockSpec((TT, D), lambda j, t: (jnp.where(j == 0, t, LAST), 0))
    cols = pl.BlockSpec((D, TT), lambda j, t: (0, jnp.where(j == 0, t, LAST)))
    tile = pl.BlockSpec((TT, FB), lambda j, t: (jnp.where(j == 0, 0, t), jnp.maximum(j - 1, 0)))
    anywhere = pl.BlockSpec(memory_space=pl.ANY)
    sems = pltpu.SemaphoreType.DMA((NJ + 1, 4, 7))
    return pl.pallas_call(
        forward_kernel,
        cost_estimate=pl.CostEstimate(flops=4 * T * D * FF, bytes_accessed=10 * T * FF, transcendentals=0),
        compiler_params=pltpu.CompilerParams(vmem_limit_bytes=VMEM_LIMIT, collective_id=3, has_side_effects=True),
        name="forward", grid=(NJ + 1, T // TT),
        in_specs=[rows, rows] + [anywhere] * 3, out_specs=[cols, cols, tile, tile, tile, anywhere, anywhere],
        out_shape=[
            jax.ShapeDtypeStruct((D, T), BF), jax.ShapeDtypeStruct((D, T), BF), jax.ShapeDtypeStruct((T, FF), F32),
            jax.ShapeDtypeStruct((T, FF), F32), jax.ShapeDtypeStruct((T, FF), BF), jax.ShapeDtypeStruct((FF, D), BF),
            jax.ShapeDtypeStruct((FF, D), BF),
        ],
        scratch_shapes=[
            pltpu.VMEM((T, D), BF), pltpu.VMEM((D, FF), BF), pltpu.VMEM((D, FF), BF), sems, sems, pltpu.SemaphoreType.DMA((4,)),
        ],
    )(x, dy, wg, wu, wd)


def down_kernel(hid_ref, x_ref, wd_ref, wg_hbm, wu_hbm, h_ref, a_ref, at_ref, wg_next, wu_next, sems, rsems, own_sems):
    me, t = lax.axis_index("s"), pl.program_id(0)
    halves = []
    for i in range(2):
        cols = pl.ds(1280 * i, 1280)
        halves.append([])
        for m in range(2):
            full = lambda k, m=m, cols=cols: block((wg_next, wu_next)[m], pl.multiple_of(flip(me, k) * 128, 128), 128, cols)
            halves[i].append(Gather(me, (wg_hbm, wu_hbm)[m].at[1, :, cols], full, ORDER[m], sems.at[i, m], rsems.at[i, m]))
    rows = pl.ds(pl.multiple_of(me * 128, 128), 128)
    own = [
        lambda: pltpu.make_async_copy(wg_hbm.at[1], wg_next.at[rows], own_sems.at[0]),
        lambda: pltpu.make_async_copy(wu_hbm.at[1], wu_next.at[rows], own_sems.at[1]),
    ]

    @pl.when(t == 0)
    def _():
        greet(me, [{"s": flip(me, k)} for k in (1, 2, 4)])
        begin(halves[0])
        begin(halves[1])
        starts(own)

    @pl.when(t == 4)
    def _():
        onward(halves[0])

    @pl.when(t == 7)
    def _():
        onward(halves[1])

    h = x_ref[...] + dot(hid_ref[...], wd_ref[...]).astype(BF)
    h_ref[...] = h
    wide = h.astype(F32)
    a = (wide * norm_scale(wide)).astype(BF)
    a_ref[...] = a
    at_ref[...] = a.T

    @pl.when(t == 7)
    def _():
        for g in halves:
            across(g)
        for g in halves:
            here(g)
            sent(g)
        for c in own:
            c().wait()


def down(hid, x, wd, wg, wu):
    rows = pl.BlockSpec((512, D), lambda t: (t, 0))
    anywhere = pl.BlockSpec(memory_space=pl.ANY)
    sems = pltpu.SemaphoreType.DMA((2, 2, 7))
    return pl.pallas_call(
        down_kernel,
        cost_estimate=pl.CostEstimate(flops=2 * T * D * FF, bytes_accessed=2 * T * FF + 8 * T * D, transcendentals=0),
        compiler_params=pltpu.CompilerParams(vmem_limit_bytes=VMEM_LIMIT, collective_id=4, has_side_effects=True),
        name="down", grid=(T // 512,),
        in_specs=[pl.BlockSpec((512, FF), lambda t: (t, 0)), rows, pl.BlockSpec((FF, D), lambda t: (0, 0)), anywhere, anywhere],
        out_specs=[rows, rows, pl.BlockSpec((D, 512), lambda t: (0, t)), anywhere, anywhere],
        out_shape=[
            jax.ShapeDtypeStruct((T, D), BF), jax.ShapeDtypeStruct((T, D), BF), jax.ShapeDtypeStruct((D, T), BF),
            jax.ShapeDtypeStruct((D, FF), BF), jax.ShapeDtypeStruct((D, FF), BF),
        ],
        scratch_shapes=[sems, sems, pltpu.SemaphoreType.DMA((2,))],
    )(hid, x, wd, wg, wu)


def cat(refs):
    return jnp.concatenate([r[...] for r in refs], axis=1)


def comm_scratch(chunks):
    blocks = (2, 2, 384, 512)
    return [
        pltpu.VMEM(blocks, F32),
        pltpu.VMEM(blocks, BF),
        pltpu.VMEM((2, *blocks), BF),
        pltpu.VMEM((2, 2, 192, 512), BF),
        pltpu.VMEM((2, 2, 2, 192, 512), BF),
        pltpu.VMEM((2, 192, 512), BF),
        pltpu.VMEM((2, 2, 192, 512), BF),
        pltpu.VMEM((384, 512), BF),
        pltpu.VMEM((2, 384, 512), BF),
        pltpu.SemaphoreType.DMA((6,)),
        pltpu.SemaphoreType.DMA((6, 2)),
    ]


def exchange(me, peer, keep, send1, recv1, send2, recv2, send3, recv3, send4, recv4, sems, rsems, out_ref):
    one, two, four = ({"s": flip(me, k)} for k in (1, 2, 4))
    z = {"r": peer}

    def copy(i, src, dst, slot, to):
        return pltpu.make_async_remote_copy(
            src_ref=src, dst_ref=dst, send_sem=sems.at[i], recv_sem=rsems.at[i, slot], device_id=to, device_id_type=pl.DeviceIdType.MESH
        )

    def c1(slot):
        return [copy(0, send1, recv1.at[slot], slot, one)]

    def c2(slot):
        return [copy(1 + i, send2.at[i], recv2.at[slot, i], slot, to) for i, to in enumerate((four, two))]

    def c3(slot):
        return [copy(3 + i, send3.at[i], recv3.at[slot, i], slot, to) for i, to in enumerate((two, four))]

    def c4(slot):
        return [copy(5, send4, recv4.at[slot], slot, z)]

    def start(cs):
        for c in cs:
            c.start()

    def wait(cs):
        for c in cs:
            c.wait()

    lo, hi = slice(0, 192), slice(192, 384)

    def s1(slot):
        start(c1(slot))

    def s2(slot):
        wait(c1(slot))
        for k in range(2):
            def total(kx, ky, rows):
                return keep[kx, ky, rows] + recv1[slot, kx, ky, rows].astype(F32)

            send2[0, k] = total(1, k, lo).astype(BF)
            send2[1, k] = total(k, 1, hi).astype(BF)
            keep[0, k, lo] = total(0, k, lo)
            keep[k, 0, hi] = total(k, 0, hi)
        start(c2(slot))

    def s3(slot):
        wait(c2(slot))
        send3[0] = (keep[0, 1, lo] + recv2[slot, 0, 1].astype(F32)).astype(BF)
        send3[1] = (keep[1, 0, hi] + recv2[slot, 1, 1].astype(F32)).astype(BF)
        keep[0, 0, lo] = keep[0, 0, lo] + recv2[slot, 0, 0].astype(F32)
        keep[0, 0, hi] = keep[0, 0, hi] + recv2[slot, 1, 0].astype(F32)
        start(c3(slot))

    def s4(slot):
        wait(c3(slot))
        send4[lo] = (keep[0, 0, lo] + recv3[slot, 0].astype(F32)).astype(BF)
        send4[hi] = (keep[0, 0, hi] + recv3[slot, 1].astype(F32)).astype(BF)
        start(c4(slot))

    def final(e, slot):
        wait(c4(slot))
        out_ref[e] = (send4[...].astype(F32) + recv4[slot].astype(F32)).astype(BF)

    return s1, s2, s3, s4, final


def grads_kernel(second, *refs):
    if second:
        a_ref, *refs = refs
        wg, wu, refs = refs[:4], refs[4:8], refs[8:]
        dy_ref, at_ref, dyt_ref, wd_ref, out_ref, dg_ref, du_ref, hkeep, hsend, accg, accu, accd, down_ref, hsems, *comm = refs
    else:
        g_refs, u_refs, refs = refs[:4], refs[4:8], refs[8:]
        dy_ref, at_ref, dyt_ref, wd_ref, hkeep, hsend, done_ref, out_ref, sums_out, units_out, *refs = refs
        accg, accu, accd, down_ref, hsems, squares, mine_ref, sums_ref, units_ref, tsems, trsems, *comm = refs
    keep, send1 = comm[:2]
    me, group = lax.axis_index("s"), lax.axis_index("r")
    j, t = pl.program_id(0), pl.program_id(1)
    last = pl.num_programs(1) - 1
    off = 0 if second else 1
    s1, s2, s3, s4, last_stage = exchange(me, 1 - group, *comm, out_ref)

    def square(v):
        v = v.astype(F32)
        squares[...] += jnp.sum((v * v).reshape(-1, 8, 512), axis=0)

    def final(e, slot):
        last_stage(e if second else e + NJ - 1, slot)
        if not second:
            square(out_ref[e + NJ - 1])

    def copy_done():
        return pltpu.make_async_copy(done_ref, out_ref.at[pl.ds(0, NJ - 1)], hsems.at[2])


    @pl.when((j == 0) & (t == 0))
    def _():
        greet(me, [{"s": flip(me, k)} for k in ((1, 2, 4) if second else range(1, 8))] + [{"r": 1 - group}])
        if not second:
            copy_done().start()
            squares[...] = jnp.zeros_like(squares)
            hands = [pltpu.make_async_copy(hkeep, keep, hsems.at[0]), pltpu.make_async_copy(hsend, send1, hsems.at[1])]
            for h in hands:
                h.start()
            for h in hands:
                h.wait()
            s1(0)

    @pl.when(t == 0)
    def _():
        for acc in (accg, accu, accd):
            acc[...] = jnp.zeros_like(acc)

    def front(i):
        two = slice(2 * i, 2 * i + 2)
        cols = slice(256 * i, 256 * (i + 1))
        if second:
            a = a_ref[...]
            g, u = dot(a, cat(wg[two])), dot(a, cat(wu[two]))
        else:
            g, u = cat(g_refs[two]), cat(u_refs[two])
        dh = dot(dy_ref[...], wd_ref[two].reshape(256, D), NT).astype(BF).astype(F32)
        s = jax.nn.sigmoid(g)
        silu = g * s
        hid = (silu * u).astype(BF)
        du = (dh * silu).astype(BF)
        dg = (dh * u * (s + silu * (1.0 - s))).astype(BF)
        if second:
            dg_ref[:, cols] = dg
            du_ref[:, cols] = du
        return hid, dg, du

    def back(i, hid, dg, du):
        cols = slice(256 * i, 256 * (i + 1))
        accg[:, cols] += dot(at_ref[...], dg)
        accu[:, cols] += dot(at_ref[...], du)
        accd[:, cols] += dot(dyt_ref[...], hid)

    zero, one = front(0), front(1)
    back(0, *zero)
    back(1, *one)

    e = j - 1 + off
    slot = lax.rem(e + 2, 2)
    for at_t, stage in ((0, s2), (2, s3), (3, s4)):
        @pl.when((t == at_t) & (e >= 0))
        def _():
            stage(slot)

    if not second:
        @pl.when((t == 1) & (j == 0))
        def _():
            copy_done().wait()
            for i in range(NJ - 1):
                square(out_ref[i])

    @pl.when((t == 1) & (e >= 1))
    def _():
        final(e - 1, lax.rem(e + 1, 2))

    @pl.when(t == last)
    def _():
        down_ref[...] = accd[...].T
        for k in range(8):
            out = (keep, send1)[k % 2]
            kx, ky = k // 4, k // 2 % 2
            d = flip(me, k)
            wide = pl.ds(pl.multiple_of(d * 128, 128), 128)
            rows = pl.ds(pl.multiple_of(d * 64, 64), 64)
            out[kx, ky, 0:128] = accg[wide, :].astype(out.dtype)
            out[kx, ky, 128:256] = accu[wide, :].astype(out.dtype)
            out[kx, ky, 256:320] = down_ref[rows, 0:512].astype(out.dtype)
            out[kx, ky, 320:384] = down_ref[rows, 512:1024].astype(out.dtype)

    new = lax.rem(e + 3, 2)
    end = (t == last) & (j == NJ - 1)
    if second:
        @pl.when((t == last) & (j < NJ - 1))
        def _():
            s1(new)

        @pl.when(end)
        def _():
            hands = [pltpu.make_async_copy(keep, hkeep, hsems.at[0]), pltpu.make_async_copy(send1, hsend, hsems.at[1])]
            for h in hands:
                h.start()
            final(NJ - 2, (NJ - 2) % 2)
            for h in hands:
                h.wait()
    else:
        @pl.when(t == last)
        def _():
            s1(new)

        @pl.when(end)
        def _():
            final(NJ - 1, (NJ - 1) % 2)
            for stage in (s2, s3, s4):
                stage(NJ % 2)
            final(NJ, NJ % 2)
            mine_ref[...] = sum(squares[:, 128 * i : 128 * (i + 1)] for i in range(4))
            sums_ref[me] = mine_ref[...]
            tails = [
                pltpu.make_async_remote_copy(
                    src_ref=mine_ref, dst_ref=sums_ref.at[me], send_sem=tsems.at[k], recv_sem=trsems.at[k],
                    device_id={"s": flip(me, k)}, device_id_type=pl.DeviceIdType.MESH,
                )
                for k in range(1, 8)
            ]
            theirs = 3 - 3 * lax.rem(me, 2)
            for layer in range(2):
                for i in range(2):
                    n = 8 + 2 * layer + i
                    tails.append(
                        pltpu.make_async_remote_copy(
                            src_ref=out_ref.at[NJ * layer + theirs + i, pl.ds(256, 128)], dst_ref=units_ref.at[layer, i],
                            send_sem=tsems.at[n], recv_sem=trsems.at[n], device_id={"s": flip(me, 1)}, device_id_type=pl.DeviceIdType.MESH,
                        )
                    )
            for c in tails:
                c.start()
            for c in tails:
                c.wait()
            sums_out[...] = sums_ref[...]
            units_out[...] = units_ref[...]


def grads(gate_up_of, dy, at, dyt, wd, handed=None):
    second = handed is None
    rows = pl.BlockSpec((TT, D), lambda j, t: (t, 0))
    cols = pl.BlockSpec((D, TT), lambda j, t: (0, t))
    if second:
        a, wg, wu = gate_up_of
        wspec = [pl.BlockSpec((D, 128), lambda j, t, c=c: (0, 5 * c + j)) for c in range(4)]
        ops, specs = [a] + [wg] * 4 + [wu] * 4, [rows] + wspec * 2
    else:
        g, u = gate_up_of
        gspec = [pl.BlockSpec((TT, 128), lambda j, t, c=c: (t, 5 * c + j)) for c in range(4)]
        ops, specs = [g] * 4 + [u] * 4, gspec * 2
    chunks = NJ - 1 if second else 2 * NJ
    ops += [dy, at, dyt, wd.reshape(4, NJ, 128, D)]
    specs += [rows, cols, cols, pl.BlockSpec((4, 1, 128, D), lambda j, t: (0, j, 0, 0))]
    outs = [jax.ShapeDtypeStruct((chunks, 384, 512), BF)]
    ospecs = [pl.BlockSpec((chunks, 384, 512), lambda j, t: (0, 0, 0))]
    tail = []
    hand = [jax.ShapeDtypeStruct((2, 2, 384, 512), F32), jax.ShapeDtypeStruct((2, 2, 384, 512), BF)]
    anywhere = [pl.BlockSpec(memory_space=pl.ANY)] * 2
    if second:
        outs += [jax.ShapeDtypeStruct((T, FF), BF)] * 2 + hand
        ospecs += [pl.BlockSpec((TT, FB), lambda j, t: (t, j))] * 2 + anywhere
    else:
        ops += handed
        specs += anywhere + anywhere[:1]
        outs += [jax.ShapeDtypeStruct((8, 8, 128), F32), jax.ShapeDtypeStruct((2, 2, 128, 512), BF)]
        ospecs += [pl.BlockSpec((8, 8, 128), lambda j, t: (0, 0, 0)), pl.BlockSpec((2, 2, 128, 512), lambda j, t: (0, 0, 0, 0))]
        tail = [pltpu.VMEM((8, 512), F32), pltpu.VMEM((8, 128), F32), pltpu.VMEM((8, 8, 128), F32), pltpu.VMEM((2, 2, 128, 512), BF), pltpu.SemaphoreType.DMA((12,)), pltpu.SemaphoreType.DMA((12,))]
    return pl.pallas_call(
        functools.partial(grads_kernel, second),
        cost_estimate=pl.CostEstimate(flops=(12 if second else 8) * T * D * FF, bytes_accessed=40 * T * D * NJ, transcendentals=0),
        compiler_params=pltpu.CompilerParams(vmem_limit_bytes=VMEM_LIMIT, collective_id=1 if second else 2, has_side_effects=True),
        name="grads_second" if second else "grads_first", grid=(NJ, T // TT),
        in_specs=specs, out_specs=ospecs, out_shape=outs,
        scratch_shapes=[pltpu.VMEM((D, FB), F32)] * 3 + [pltpu.VMEM((FB, D), F32), pltpu.SemaphoreType.DMA((3,))] + tail + comm_scratch(chunks),
    )(*ops)


def dstate_kernel(groups, *refs):
    n = len(groups)
    dgs, dus, (h_ref, dy_ref, wg_ref, wu_ref, dh_ref, dht_ref) = refs[:n], refs[n : 2 * n], refs[2 * n :]

    def back(parts, w_ref):
        total, j = None, 0
        for ref, count in zip(parts, groups, strict=True):
            for k in range(count):
                w = jnp.concatenate([w_ref[:, 128 * (5 * c + j) : 128 * (5 * c + j + 1)] for c in range(4)], axis=1)
                one = dot(ref[:, FB * k : FB * (k + 1)], w, NT)
                total = one if total is None else total + one
                j += 1
        return total.astype(BF)

    da = (back(dgs, wg_ref) + back(dus, wu_ref)).astype(F32)
    wide = h_ref[...].astype(F32)
    scale = norm_scale(wide)
    along = jnp.sum(da * wide, -1, keepdims=True)
    dn = (da * scale - wide * (along * scale * scale * scale * (1.0 / D))).astype(BF)
    dh = dy_ref[...] + dn
    dh_ref[...] = dh
    dht_ref[...] = dh.T


def dstate(dgs, dus, h, dy, wg, wu):
    groups = tuple(d.shape[1] // FB for d in dgs)
    tt = 512
    rows = pl.BlockSpec((tt, D), lambda t: (t, 0))
    wide = [pl.BlockSpec((tt, FB * n), lambda t: (t, 0)) for n in groups]
    w = pl.BlockSpec((D, FF), lambda t: (0, 0))
    return call(
        functools.partial(dstate_kernel, groups), 4 * T * D * FF, 4 * T * FF + 8 * T * D, name="dstate", grid=(T // tt,),
        in_specs=wide * 2 + [rows, rows, w, w],
        out_specs=[rows, pl.BlockSpec((D, tt), lambda t: (0, t))],
        out_shape=[jax.ShapeDtypeStruct((T, D), BF), jax.ShapeDtypeStruct((D, T), BF)],
    )(*dgs, *dus, h, dy, wg, wu)


def update_kernel(g_ref, units_ref, sums_ref, *refs):
    ins, outs = refs[:9], refs[9:]
    layer, q = pl.program_id(0), pl.program_id(1)
    core = lax.rem(lax.axis_index("s"), 2)
    base = NJ * (1 - layer)
    factor = jnp.minimum(1.0, 0.5 * lax.rsqrt(jnp.sum(sums_ref[...], keepdims=True)[0] * (1.0 / (3 * 2 * D * FF)) + 1e-30))

    def wide(first):
        parts = []
        for b in range(4):
            n = 4 * q + b
            chip, c = lax.div(n, NJ), lax.rem(n, NJ)
            parts.append(g_ref[base + c, first : first + 128, pl.ds(pl.multiple_of(chip * 128, 128), 128)])
        return jnp.concatenate(parts, axis=1)

    half = lax.div(q, 2)
    own = g_ref[base + half + 2 * core, 256:384].astype(F32)
    other = units_ref[1 - layer, jnp.minimum(half, 1)].astype(F32)
    unit = jnp.where(lax.rem(q, 2) == 0, own, other)
    grads = [wide(0).astype(F32), wide(128).astype(F32), jnp.concatenate([unit[:64], unit[64:]], axis=1)]
    for i, g in enumerate(grads):
        g = g * factor
        w, m, v = (ins[3 * n + i][0].astype(F32) for n in range(3))
        m = 0.9 * m + 0.1 * g
        v = 0.95 * v + 0.05 * g * g
        step = m * lax.rsqrt(v + 1e-8) + 0.1 * w
        outs[i][0] = (w - 0.02 * step).astype(BF)
        outs[3 + i][0] = m
        outs[6 + i][0] = v


def update(g, units, sums, arrays):
    wide = pl.BlockSpec((1, 128, 512), lambda l, q: (l, 0, q))
    tall = pl.BlockSpec((1, 64, D), lambda l, q: (l, q, 0))
    specs = [wide, wide, tall] * 3
    whole = [pl.BlockSpec(v.shape, lambda l, q, n=v.ndim: (0,) * n) for v in (g, units, sums)]
    return pl.pallas_call(
        update_kernel,
        cost_estimate=pl.CostEstimate(flops=10 * 6 * D * FF // 8, bytes_accessed=20 * 6 * D * FF // 8, transcendentals=0),
        compiler_params=pltpu.CompilerParams(vmem_limit_bytes=VMEM_LIMIT),
        name="update", grid=(2, NJ), in_specs=whole + specs, out_specs=specs,
        out_shape=[jax.ShapeDtypeStruct(v.shape, v.dtype) for v in arrays],
    )(g, units, sums, *arrays)


def solution(mesh):
    def step(x, dy, *arrays):
        weights, x, dy = arrays[:3], x[0], dy[0]
        wg, wu, wd = weights
        a0t, dyt, g0, u0, hid0, wd0, wd1 = forward(x, dy, *weights)
        h1, a1, a1t, wg1, wu1 = down(hid0, x, wd0, wg, wu)
        done1, dg, du, *handed = grads((a1, wg1, wu1), dy, a1t, dyt, wd1)
        dh1, dh1t = dstate([dg], [du], h1, dy, wg1, wu1)
        done, sums, units = grads((g0, u0), dh1, a0t, dh1t, wd0, handed + [done1])
        return tuple(update(done, units, sums, arrays))

    states, cut = P(("rep", "r", "s"), None, None), P(None, "s", None)
    return jax.shard_map(
        step, mesh=mesh, in_specs=(states, states) + (cut,) * 9, out_specs=(P("rep", "s", None),) * 9, check_vma=False,
    )
```
